32 devices in a mesh: scen: 16 (over z, y, x), fac: 2 (over core).
Axes of the slice: x: 2, y: 2, z: 4, core: 2. Of those that a mesh axis runs over, the one named last changes fastest.
Arguments:
- scenario_pnl: float32 [16384, 2048], P('scen', 'fac'), may hold values from -300 to 300
Outputs:
- covariance: float32 [2048, 2048], P('scen', 'fac')
- factor_means: float32 [2048], P('fac')
The draws below stay inside these ranges and needn't reach their ends.
All inputs are finite; a program needn't handle non-finite values.
Results may differ from the reference program's by a relative error of at most 0.0003.
Values sent between devices are 32-bit elements; how exact they have to be, the bound alone decides.
A program may use at most 64 MiB of HBM per device.

```python
import jax
import jax.numpy as jnp
from jax import lax

F = 2048
SCENARIOS = 16384


def draw_scenario_pnl(key, part):
    keys = jax.random.split(jax.random.fold_in(key, 11), 9)
    noise = jnp.clip(jax.random.normal(keys[0], (SCENARIOS, F), jnp.float32), -4.0, 4.0)
    first = jax.random.permutation(keys[1], F)
    second = jax.random.permutation(keys[2], F)
    mixed = noise + 0.5 * noise[:, first] + 0.5 * noise[:, second]
    levels = jnp.clip(0.8 * jax.random.normal(keys[3], (F,), jnp.float32), -2.0, 2.0)
    scales = jnp.exp(jax.random.uniform(keys[4], (F,), jnp.float32, jnp.log(0.4), jnp.log(2.5)))
    drift = 0.5 + jnp.arange(SCENARIOS, dtype=jnp.float32) / SCENARIOS
    drawn = scales[None, :] * (mixed + drift[:, None] * levels[None, :])
    chosen = jax.random.permutation(keys[6], F) < F // 8
    signs = jnp.where(jax.random.uniform(keys[7], (F,), jnp.float32) < 0.5, -1.0, 1.0)
    offsets = signs * jax.random.uniform(keys[8], (F,), jnp.float32, 200.0, 260.0)
    shifted = offsets[None, :] + mixed + 2.0 * (drift[:, None] - 1.0)
    return jnp.where(chosen[None, :], shifted, drawn)


def setup_inputs(seed: int = 0) -> dict:
    key_of = jax.random.split(jax.random.key(seed), 2)
    return {
        "scenario_pnl": draw_scenario_pnl(jax.random.fold_in(key_of[1], 71), 0),
    }


def reference(scenario_pnl):
    count = scenario_pnl.shape[0]
    factor_means = jnp.sum(scenario_pnl, axis=0) / count
    centered = scenario_pnl - factor_means[None, :]
    product = lax.dot_general(centered, centered, (((0,), (0,)), ((), ())), precision=lax.Precision.HIGHEST, preferred_element_type=jnp.float32)
    covariance = product / (count - 1)
    return covariance, factor_means
```

```python
import functools

import jax
import jax.numpy as jnp
from jax import lax
from jax.experimental import pallas as pl
from jax.experimental.pallas import tpu as pltpu
from jax.sharding import PartitionSpec as P

MESH = pl.DeviceIdType.MESH
LOADS = 4
TILE = 64


def block_gram(left, right):
    return lax.dot_general(
        left,
        right,
        (((0,), (0,)), ((), ())),
        precision=lax.Precision.HIGHEST,
        preferred_element_type=jnp.float32,
    )


def on_device(scenario_pnl):
    rows_here = scenario_pnl.shape[0]
    total_rows = rows_here * lax.axis_size("scen")
    local_sums = jnp.sum(scenario_pnl, axis=0)
    total_sums = lax.psum(local_sums, "scen")
    factor_means = total_sums / total_rows
    local_means = local_sums / rows_here
    data = scenario_pnl - local_means[None, :]
    partial_value = block_gram(lax.all_gather(data, "fac", axis=1, tiled=True), data)
    owned = lax.psum_scatter(partial_value, "scen", scatter_dimension=0, tiled=True)
    gathered = lax.all_gather(local_means, ("scen", "fac"), axis=0, tiled=True)
    spread_rows = gathered.reshape(lax.axis_size("scen"), -1)
    deviations = spread_rows - jnp.mean(spread_rows, axis=0, keepdims=True)
    owned_rows = owned.shape[0]
    column_width = owned.shape[1]
    row_part = lax.dynamic_slice_in_dim(
        deviations, lax.axis_index("scen") * owned_rows, owned_rows, 1
    )
    column_part = lax.dynamic_slice_in_dim(
        deviations, lax.axis_index("fac") * column_width, column_width, 1
    )
    owned = owned + rows_here * block_gram(row_part, column_part)
    covariance = owned / (total_rows - 1)
    return (covariance, factor_means)


def kernel(
    n, x_hbm, cov_ref, mean_ref,
    x_vm, other, hi_w, lo_w, hi_o, lo_o,
    send1, keep1, recv1, send2, recv2, zsend, zrecv,
    turned, landed, sums_own, sums_oth, dev_w, dev_o,
    load_sem, pair_s, pair_r, s1_s, s1_r, s2_s, s2_r, z_s, z_r, t_s, t_r,
    m_s, m_r, mo_s, mo_r,
):
    rows, width = x_hbm.shape
    half = n // 2
    block = width // half
    near, far = half // 2 + 1, half // 2
    depth = n // 4
    zh = depth // 2
    total_rows = rows * n

    s = lax.axis_index("scen")
    c = lax.axis_index("fac")
    z, y, x = s // 4, (s // 2) % 2, s % 2
    first = x * (1 - c) + y * c
    second = y * (1 - c) + x * c
    peer1 = s + (1 - 2 * x) * (1 - c) + (2 - 4 * y) * c
    peer2 = s + (2 - 4 * y) * (1 - c) + (1 - 2 * x) * c

    barrier = pltpu.get_barrier_semaphore()
    me = s * 2 + c

    part = rows // LOADS
    loads = []
    for i in range(LOADS):
        at = pl.ds(i * part, part)
        load = pltpu.make_async_copy(x_hbm.at[at], x_vm.at[at], load_sem.at[i])
        load.start()
        loads.append(load)

    def greet(d, carry):
        p = (me + d) % (2 * n)
        pl.semaphore_signal(barrier, inc=1, device_id=(p // 2, p % 2), device_id_type=MESH)
        return carry

    lax.fori_loop(1, 2 * n, greet, 0)

    def sums_of(ref, start, count, acc):
        def add(i, acc):
            at = pl.multiple_of(start + i * TILE, TILE)
            return acc + jnp.sum(ref[pl.ds(at, TILE), :].reshape(TILE // 8, 8, width), axis=0)

        return lax.fori_loop(0, count // TILE, add, acc)

    acc = jnp.zeros((8, width), jnp.float32)
    for i in range(LOADS):
        loads[i].wait()
        acc = sums_of(x_vm, i * part, part, acc)
    local_sum = jnp.sum(acc, axis=0, keepdims=True)
    sums_own[s] = local_sum
    local_mean = local_sum / rows
    mid = width // 2

    def split_own(i, carry):
        at = pl.ds(pl.multiple_of(i * TILE, TILE), TILE)
        data = x_vm[at, :] - local_mean
        hi = data.astype(jnp.bfloat16)
        lo = (data - hi.astype(jnp.float32)).astype(jnp.bfloat16)
        hi_w[at, :width] = hi
        lo_w[at, :width] = lo
        hi_w[at, width:] = hi[:, :mid]
        lo_w[at, width:] = lo[:, :mid]
        return carry

    lax.fori_loop(0, rows // TILE, split_own, 0)

    def split_other():
        acc = sums_of(other, 0, rows, jnp.zeros((8, width), jnp.float32))
        mean = jnp.sum(acc, axis=0, keepdims=True) / rows

        def body(i, carry):
            at = pl.ds(pl.multiple_of(i * TILE, TILE), TILE)
            data = other[at, :] - mean
            hi = data.astype(jnp.bfloat16)
            hi_o[at, :] = hi
            lo_o[at, :] = (data - hi.astype(jnp.float32)).astype(jnp.bfloat16)
            return carry

        lax.fori_loop(0, rows // TILE, body, 0)

    def gram(left, right):
        return lax.dot_general(
            left, right, (((0,), (0,)), ((), ())), preferred_element_type=jnp.float32
        )

    def slot_of(k):
        turn = (k + z) % zh
        return c * zh + turn if k < zh else (1 - c) * zh + turn

    def width_of(k):
        return (near if k < zh else far) * block

    def compute(k, side, dst, send=False):
        own = k < zh
        wide = width_of(k)
        hi_l, lo_l = (hi_w, lo_w) if own else (hi_o, lo_o)

        def body(j, carry):
            b = (1 - second) + j * (2 * second - 1)
            px = side * (1 - c) + b * c
            py = b * (1 - c) + side * c
            r = (slot_of(k) * 4 + py * 2 + px) % half
            rows_at = pl.ds(pl.multiple_of(r * block, block), block)
            start = r if own else r + c
            cols_at = pl.ds(pl.multiple_of(start * block, block), wide)
            lh, ll = hi_l[:, rows_at], lo_l[:, rows_at]
            rh, rl = hi_w[:, cols_at], lo_w[:, cols_at]
            dst[k, j, :, :wide] = gram(lh, rh) + (gram(lh, rl) + gram(ll, rh))
            if send:
                stage1(k, j).start()
            return carry

        lax.fori_loop(0, 2, body, 0)

    def remote(src, dst, send, recv, scen, fac):
        return pltpu.make_async_remote_copy(
            src_ref=src, dst_ref=dst, send_sem=send, recv_sem=recv,
            device_id=(scen, fac), device_id_type=MESH,
        )

    def stage1(k, j):
        w = width_of(k)
        return remote(
            send1.at[k, j, :, :w], recv1.at[k, j, :, :w], s1_s.at[k, j], s1_r.at[k, j], peer1, c
        )

    def stage2(k):
        w = width_of(k)
        return remote(send2.at[k, :, :w], recv2.at[k, :, :w], s2_s.at[k], s2_r.at[k], peer2, c)

    def stage3(k):
        w = width_of(k)
        t = slot_of(k)
        place = (z - t + depth - 1) % depth
        return remote(
            zsend.at[k, :, :w], zrecv.at[place, :, :w], z_s.at[k], z_r.at[place],
            t * 4 + y * 2 + x, c,
        )

    def relay1(k):
        w = width_of(k)
        stage1(k, 0).wait_recv()
        send2[k, :, :w] = keep1[k, 0, :, :w] + recv1[k, 0, :, :w]
        stage2(k).start()

    def relay2(k):
        w = width_of(k)
        stage1(k, 1).wait_recv()
        stage2(k).wait_recv()
        zsend[k, :, :w] = keep1[k, 1, :, :w] + recv1[k, 1, :, :w] + recv2[k, :, :w]

        @pl.when(slot_of(k) != z)
        def _():
            stage3(k).start()

    pl.semaphore_wait(barrier, 2 * n - 1)
    compute(0, 1 - first, send1, True)
    pair = remote(x_vm, other, pair_s, pair_r, s, 1 - c)
    pair.start()

    def mean_copy(d):
        p = (s + d) % n
        return remote(sums_own.at[s], sums_own.at[s], m_s.at[d], m_r.at[d], p, c)

    for d in range(1, n):
        mean_copy(d).start()

    compute(0, first, keep1)
    compute(1, 1 - first, send1, True)
    compute(1, first, keep1)

    for d in range(1, n):
        q = (s - d + n) % n
        remote(sums_own.at[q], sums_own.at[q], m_s.at[d], m_r.at[d], q, c).wait_recv()
    swap = remote(sums_own, sums_oth, mo_s, mo_r, s, 1 - c)
    swap.start()

    relay1(0)
    pair.wait_recv()
    split_other()
    compute(2, 1 - first, send1, True)
    relay1(1)
    compute(2, first, keep1)
    compute(3, 1 - first, send1, True)
    relay2(0)
    compute(3, first, keep1)

    def deviations(ref):
        sums = ref[...].reshape(n, width)
        total = jnp.sum(sums, axis=0, keepdims=True)
        return sums / rows - total / total_rows, total / total_rows

    dev, means = deviations(sums_own)
    mean_ref[...] = means
    dev_w[:, :width] = dev
    dev_w[:, width:] = dev[:, :mid]
    swap.wait_recv()
    dev_o[...] = deviations(sums_oth)[0]

    relay1(2)
    relay2(1)
    relay1(3)
    relay2(2)
    relay2(3)

    r = s % half

    def turn_copy(own, d):
        if own:
            return remote(
                turned.at[d], landed.at[d], t_s.at[d], t_r.at[d], c * half + (r + d) % half, c
            )
        return remote(
            turned.at[d], landed.at[d], t_s.at[d], t_r.at[d],
            c * half + (r + c + d) % half, 1 - c,
        )

    def finish(own):
        count = near if own else far
        w = count * block
        for k in (range(zh) if own else range(zh, 2 * zh)):
            @pl.when(slot_of(k) == z)
            def _():
                for place in range(depth - 1):
                    remote(
                        zsend.at[k, :, :w], zrecv.at[place, :, :w], z_s.at[k], z_r.at[place],
                        s, 1 - c,
                    ).wait_recv()
                left = (dev_w if own else dev_o)[:, pl.ds(pl.multiple_of(r * block, block), block)]
                start = r if own else r + c
                shift = block_gram(
                    left, dev_w[:, pl.ds(pl.multiple_of(start * block, block), w)]
                )
                value = zsend[k, :, :w]
                for place in range(depth - 1):
                    value = value + zrecv[place, :, :w]
                value = (value + rows * shift) / (total_rows - 1)
                turns = range(1, near - 1) if own else range(far)
                for d in turns:
                    turned[d] = value[:, d * block:(d + 1) * block].T
                    turn_copy(own, d).start()
                for d in range(count):
                    q = (start + d) % half
                    cov_ref[:, pl.ds(pl.multiple_of(q * block, block), block)] = value[
                        :, d * block:(d + 1) * block
                    ]
                for d in turns:
                    turn_copy(own, d).wait_recv()
                    q = (r - d + half) % half if own else (r - (1 - c) - d + 2 * half) % half
                    cov_ref[:, pl.ds(pl.multiple_of(q * block, block), block)] = landed[d]
                for d in turns:
                    turn_copy(own, d).wait_send()

    finish(True)
    finish(False)

    pair.wait_send()
    swap.wait_send()
    for d in range(1, n):
        mean_copy(d).wait_send()
    for k in range(2 * zh):
        stage1(k, 0).wait_send()
        stage1(k, 1).wait_send()
        stage2(k).wait_send()

        @pl.when(slot_of(k) != z)
        def _():
            stage3(k).wait_send()


def by_kernel(n, scenario_pnl):
    rows, width = scenario_pnl.shape
    half = n // 2
    block = width // half
    near = half // 2 + 1
    depth = n // 4
    f32, bf16 = jnp.float32, jnp.bfloat16
    dma = pltpu.SemaphoreType.DMA
    covariance, factor_means = pl.pallas_call(
        functools.partial(kernel, n),
        out_shape=(pltpu.VMEM((block, width), f32), pltpu.VMEM((1, width), f32)),
        in_specs=[pl.BlockSpec(memory_space=pl.ANY)],
        out_specs=[pl.BlockSpec(memory_space=pltpu.VMEM)] * 2,
        scratch_shapes=[
            pltpu.VMEM((rows, width), f32),
            pltpu.VMEM((rows, width), f32),
            pltpu.VMEM((rows, width + width // 2), bf16),
            pltpu.VMEM((rows, width + width // 2), bf16),
            pltpu.VMEM((rows, width), bf16),
            pltpu.VMEM((rows, width), bf16),
            pltpu.VMEM((depth, 2, block, near * block), f32),
            pltpu.VMEM((depth, 2, block, near * block), f32),
            pltpu.VMEM((depth, 2, block, near * block), f32),
            pltpu.VMEM((depth, block, near * block), f32),
            pltpu.VMEM((depth, block, near * block), f32),
            pltpu.VMEM((depth, block, near * block), f32),
            pltpu.VMEM((depth - 1, block, near * block), f32),
            pltpu.VMEM((near - 1, block, block), f32),
            pltpu.VMEM((near - 1, block, block), f32),
            pltpu.VMEM((n, 1, width), f32),
            pltpu.VMEM((n, 1, width), f32),
            pltpu.VMEM((n, width + width // 2), f32),
            pltpu.VMEM((n, width), f32),
            dma((LOADS,)),
            dma, dma,
            dma((depth, 2)), dma((depth, 2)),
            dma((depth,)), dma((depth,)),
            dma((depth,)), dma((depth - 1,)),
            dma((near - 1,)), dma((near - 1,)),
            dma((n,)), dma((n,)),
            dma, dma,
        ],
        compiler_params=pltpu.CompilerParams(
            collective_id=0, has_side_effects=True, vmem_limit_bytes=60 * 1024 * 1024
        ),
    )(scenario_pnl)
    return covariance, factor_means.reshape(width)


def solution(mesh):
    n, cores = mesh.shape["scen"], mesh.shape["fac"]

    def body(scenario_pnl):
        rows, width = scenario_pnl.shape
        fits = cores == 2 and n % 16 == 0 and n // 4 == 4 and width % (n * 64) == 0
        if fits and rows % (LOADS * TILE) == 0:
            return by_kernel(n, scenario_pnl)
        return on_device(scenario_pnl)

    return jax.shard_map(
        body,
        mesh=mesh,
        in_specs=(P("scen", "fac"),),
        out_specs=(P("scen", "fac"), P("fac")),
        check_vma=False,
    )
```

```python
import functools

import jax
import jax.numpy as jnp
from jax import lax
from jax.experimental import pallas as pl
from jax.experimental.pallas import tpu as pltpu
from jax.sharding import PartitionSpec as P

MESH = pl.DeviceIdType.MESH
LOADS = 4
TILE = 64


def block_gram(left, right):
    return lax.dot_general(
        left,
        right,
        (((0,), (0,)), ((), ())),
        precision=lax.Precision.HIGHEST,
        preferred_element_type=jnp.float32,
    )


def on_device(scenario_pnl):
    rows_here = scenario_pnl.shape[0]
    total_rows = rows_here * lax.axis_size("scen")
    local_sums = jnp.sum(scenario_pnl, axis=0)
    total_sums = lax.psum(local_sums, "scen")
    factor_means = total_sums / total_rows
    local_means = local_sums / rows_here
    data = scenario_pnl - local_means[None, :]
    partial_value = block_gram(lax.all_gather(data, "fac", axis=1, tiled=True), data)
    owned = lax.psum_scatter(partial_value, "scen", scatter_dimension=0, tiled=True)
    gathered = lax.all_gather(local_means, ("scen", "fac"), axis=0, tiled=True)
    spread_rows = gathered.reshape(lax.axis_size("scen"), -1)
    deviations = spread_rows - jnp.mean(spread_rows, axis=0, keepdims=True)
    owned_rows = owned.shape[0]
    column_width = owned.shape[1]
    row_part = lax.dynamic_slice_in_dim(
        deviations, lax.axis_index("scen") * owned_rows, owned_rows, 1
    )
    column_part = lax.dynamic_slice_in_dim(
        deviations, lax.axis_index("fac") * column_width, column_width, 1
    )
    owned = owned + rows_here * block_gram(row_part, column_part)
    covariance = owned / (total_rows - 1)
    return (covariance, factor_means)


def kernel(
    n, x_hbm, cov_ref, mean_ref,
    x_vm, other, hi, lo,
    send1, keep1, recv1, send2, recv2, zsend, zrecv, xrecv,
    turned, landed, sums_own, sums_oth, pair_sum, dev_a,
    load_sem, pair_s, pair_r, ps_s, ps_r, s1_s, s1_r, s2_s, s2_r, z_s, z_r, x_s, x_r,
    t_s, t_r, m_s, m_r, mo_s, mo_r,
):
    rows, width = x_hbm.shape
    half = n // 2
    block = width // half
    quads, parts = n // 4, 2
    wide = half // 4 * block
    extra = parts * quads
    wrapped = width + width // 2
    total_rows = rows * n

    s = lax.axis_index("scen")
    c = lax.axis_index("fac")
    z, y, x = s // 4, (s // 2) % 2, s % 2
    first = x * (1 - c) + y * c
    second = y * (1 - c) + x * c
    peer1 = s + (1 - 2 * x) * (1 - c) + (2 - 4 * y) * c
    peer2 = s + (2 - 4 * y) * (1 - c) + (1 - 2 * x) * c
    odd, own_z = z % 2, 1 - (z // 2 - c) * (z // 2 - c)

    barrier = pltpu.get_barrier_semaphore()
    me = s * 2 + c

    part = rows // LOADS
    loads = []
    for i in range(LOADS):
        at = pl.ds(i * part, part)
        load = pltpu.make_async_copy(x_hbm.at[at], x_vm.at[at], load_sem.at[i])
        load.start()
        loads.append(load)

    for d in range(1, 2 * n):
        p = (me + d) % (2 * n)
        pl.semaphore_signal(barrier, inc=1, device_id=(p // 2, p % 2), device_id_type=MESH)

    def sums_of(ref, start, count, acc):
        def add(i, acc):
            at = pl.multiple_of(start + i * TILE, TILE)
            return acc + jnp.sum(ref[pl.ds(at, TILE), :].reshape(TILE // 8, 8, width), axis=0)

        return lax.fori_loop(0, count // TILE, add, acc)

    acc = jnp.zeros((8, width), jnp.float32)
    for i in range(LOADS):
        loads[i].wait()
        acc = sums_of(x_vm, i * part, part, acc)
    local_sum = jnp.sum(acc, axis=0, keepdims=True)
    sums_own[s] = local_sum
    mid = width // 2

    def split(ref, mean, base, start, count, wrap):
        def body(i, carry):
            at = pl.ds(pl.multiple_of(start + i * TILE, TILE), TILE)
            data = ref[at, :] - mean
            high = data.astype(jnp.bfloat16)
            low = (data - high.astype(jnp.float32)).astype(jnp.bfloat16)
            hi[at, base:base + width] = high
            lo[at, base:base + width] = low
            if wrap:
                hi[at, width:wrapped] = high[:, :mid]
                lo[at, width:wrapped] = low[:, :mid]
            return carry

        lax.fori_loop(0, count // TILE, body, 0)

    split(x_vm, local_sum / rows, 0, 0, rows, True)

    def gram(left, right):
        return lax.dot_general(
            left, right, (((0,), (0,)), ((), ())), preferred_element_type=jnp.float32
        )

    def slot_of(k):
        near = (z + 1 - 2 * odd, 2 * (1 - c) + odd, 3 - 2 * c - odd, z)[k]
        far = (2 * c + odd, 2 * c + 1 - odd, z + 1 - 2 * odd, z)[k]
        return own_z * near + (1 - own_z) * far

    def width_of(t):
        return block if t == extra else wide

    def strip(t, px, py):
        if t == extra:
            r = py * 2 + px
            return r, r + half // 2
        to = slot_of(t % quads)
        r = (to * 4 + py * 2 + px) % half
        own = 1 - (to // 2 - c) * (to // 2 - c)
        return r + (1 - own) * (wrapped // block), r + (1 - own) * c + t // quads * (wide // block)

    def lanes(start, count):
        return pl.ds(pl.multiple_of(start * block, block), count)

    def compute(k, side, dst, send=False):
        pieces = (extra,) if k == quads else (k, quads + k)
        count = sum(width_of(t) for t in pieces)

        def body(j, carry):
            b = (1 - second) + j * (2 * second - 1)
            px, py = side * (1 - c) + b * c, b * (1 - c) + side * c
            left, right = strip(pieces[0], px, py)
            rows_at, cols_at = lanes(left, block), lanes(right, count)
            lh, ll = hi[:, rows_at], lo[:, rows_at]
            rh, rl = hi[:, cols_at], lo[:, cols_at]
            value = gram(lh, rh) + (gram(lh, rl) + gram(ll, rh))
            for t in pieces:
                w = width_of(t)
                at = (t // quads) * wide % count
                dst[t, j, :, :w] = value[:, at:at + w]
            if send:
                stage1(pieces[0], j).start()
            return carry

        lax.fori_loop(0, 2, body, 0)

    def remote(src, dst, send, recv, scen, fac):
        return pltpu.make_async_remote_copy(
            src_ref=src, dst_ref=dst, send_sem=send, recv_sem=recv,
            device_id=(scen, fac), device_id_type=MESH,
        )

    def stage1(t, j):
        w = width_of(t)
        return remote(
            send1.at[t, j, :, :w], recv1.at[t, j, :, :w], s1_s.at[t, j], s1_r.at[t, j], peer1, c
        )

    def stage2(t):
        w = width_of(t)
        return remote(send2.at[t, :, :w], recv2.at[t, :, :w], s2_s.at[t], s2_r.at[t], peer2, c)

    def stage3(t):
        to = slot_of(t % quads)
        place = (z - to + quads - 1) % quads
        return remote(
            zsend.at[t], zrecv.at[t // quads, place], z_s.at[t], z_r.at[t // quads, place],
            to * 4 + y * 2 + x, c,
        )

    def stage3_extra(e):
        to = 2 * c + e
        place = (z - to + quads - 1) % quads
        return remote(
            zsend.at[extra, :, :block], xrecv.at[place], x_s.at[e], x_r.at[place],
            to * 4 + y * 2 + x, c,
        )

    def relay1(t):
        w = width_of(t)
        stage1(t, 0).wait_recv()
        send2[t, :, :w] = keep1[t, 0, :, :w] + recv1[t, 0, :, :w]
        stage2(t).start()

    def relay2(t):
        w = width_of(t)
        stage1(t, 1).wait_recv()
        stage2(t).wait_recv()
        zsend[t, :, :w] = keep1[t, 1, :, :w] + recv1[t, 1, :, :w] + recv2[t, :, :w]
        if t == extra:
            for e in range(2):
                @pl.when(2 * c + e != z)
                def _():
                    stage3_extra(e).start()
        elif t % quads < quads - 1:
            stage3(t).start()

    def send_stage(t):
        for j in range(2):
            stage1(t, j).start()

    def pair_copy(i):
        at = pl.ds(i * part, part)
        return remote(x_vm.at[at], other.at[at], pair_s.at[i], pair_r.at[i], s, 1 - c)

    def mean_copy(d):
        p = (s + d) % n
        return remote(sums_own.at[s], sums_own.at[s], m_s.at[d], m_r.at[d], p, c)

    pl.semaphore_wait(barrier, 2 * n - 1)
    pair_mean = remote(sums_own.at[s], pair_sum, ps_s, ps_r, s, 1 - c)
    pair_mean.start()
    for i in range(LOADS):
        pair_copy(i).start()
    compute(quads, 1 - first, send1, True)
    compute(0, 1 - first, send1, True)
    for d in range(1, n):
        mean_copy(d).start()
    send_stage(quads)
    compute(quads, first, keep1)
    compute(0, first, keep1)
    relay1(extra)

    pair_mean.wait_recv()
    pair_mean_value = pair_sum[...] / rows
    for i in range(LOADS):
        pair_copy(i).wait_recv()
        split(other, pair_mean_value, wrapped, i * part, part, False)

    compute(1, 1 - first, send1, True)
    relay1(0)
    compute(1, first, keep1)
    compute(2, 1 - first, send1, True)
    relay2(extra)
    compute(2, first, keep1)
    relay1(quads)
    compute(3, 1 - first, send1, True)
    for t in range(quads + 1, 2 * quads):
        send_stage(t)
    compute(3, first, keep1)
    relay2(0)
    relay1(1)
    for d in range(1, n):
        q = (s - d + n) % n
        remote(sums_own.at[q], sums_own.at[q], m_s.at[d], m_r.at[d], q, c).wait_recv()
    swap = remote(sums_own, sums_oth, mo_s, mo_r, s, 1 - c)
    swap.start()
    relay2(quads)
    relay1(2)
    relay2(1)
    relay1(3)
    relay2(2)

    def deviations(ref):
        sums = ref[...].reshape(n, width)
        total = jnp.sum(sums, axis=0, keepdims=True)
        return sums / rows - total / total_rows, total / total_rows

    dev, means = deviations(sums_own)
    mean_ref[...] = means
    dev_a[:, :width] = dev
    dev_a[:, width:wrapped] = dev[:, :mid]
    swap.wait_recv()
    dev_a[:, wrapped:] = deviations(sums_oth)[0]

    relay1(quads + 1)
    relay2(3)

    r = s % half
    start = r + (1 - own_z) * c

    def put(q, value):
        cov_ref[:, lanes(q % half, block)] = value

    def turn_copy(d):
        return remote(
            turned.at[d], landed.at[d], t_s.at[d], t_r.at[d],
            c * half + (start + d) % half, own_z * c + (1 - own_z) * (1 - c),
        )

    def mirrored(d, act):
        if d:
            act()
        else:
            pl.when(own_z == 0)(act)

    def finish(p):
        t = p * quads + quads - 1
        for place in range(quads - 1):
            remote(
                zsend.at[t], zrecv.at[p, place], z_s.at[t], z_r.at[p, place], s, 1 - c
            ).wait_recv()
        left, right = strip(t, x, y)
        shift = block_gram(dev_a[:, lanes(left, block)], dev_a[:, lanes(right, wide)])
        value = zsend[t]
        for place in range(quads - 1):
            value = value + zrecv[p, place]
        value = (value + rows * shift) / (total_rows - 1)
        each = wide // block
        for i in range(each):
            d = p * each + i
            turned[d] = value[:, i * block:(i + 1) * block].T
            mirrored(d, turn_copy(d).start)
        for i in range(each):
            put(start + p * each + i, value[:, i * block:(i + 1) * block])

    def land(p):
        for d in range(p * (wide // block), (p + 1) * (wide // block)):
            def arrive():
                turn_copy(d).wait_recv()
                put(r - (1 - own_z) * (1 - c) - d + 2 * half, landed[d])

            mirrored(d, arrive)

    def finish_extra():
        @pl.when(own_z == 1)
        def _():
            for place in range(quads - 1):
                remote(
                    zsend.at[extra, :, :block], xrecv.at[place], x_s.at[0], x_r.at[place], s, 1 - c
                ).wait_recv()
            left, right = strip(extra, x, y)
            shift = block_gram(dev_a[:, lanes(left, block)], dev_a[:, lanes(right, block)])
            value = zsend[extra, :, :block]
            for place in range(quads - 1):
                value = value + xrecv[place]
            value = (value + rows * shift) / (total_rows - 1)

            @pl.when(odd == 0)
            def _():
                put(r + half // 2, value)

            @pl.when(odd == 1)
            def _():
                put(r + half // 2, value.T)

    relay1(quads + 2)
    relay2(quads + 1)
    relay1(quads + 3)
    relay2(quads + 2)
    finish(0)
    finish_extra()
    relay2(quads + 3)
    finish(1)
    land(0)
    land(1)

    pair_mean.wait_send()
    for i in range(LOADS):
        pair_copy(i).wait_send()
    swap.wait_send()
    for d in range(1, n):
        mean_copy(d).wait_send()
    for d in range(half // 2):
        mirrored(d, turn_copy(d).wait_send)
    for t in range(extra + 1):
        stage1(t, 0).wait_send()
        stage1(t, 1).wait_send()
        stage2(t).wait_send()
        if t == extra:
            for e in range(2):
                @pl.when(2 * c + e != z)
                def _():
                    stage3_extra(e).wait_send()
        elif t % quads < quads - 1:
            stage3(t).wait_send()


def by_kernel(n, scenario_pnl):
    rows, width = scenario_pnl.shape
    half = n // 2
    block = width // half
    wide = half // 4 * block
    tasks = 2 * (n // 4) + 1
    f32, bf16 = jnp.float32, jnp.bfloat16
    dma = pltpu.SemaphoreType.DMA
    covariance, factor_means = pl.pallas_call(
        functools.partial(kernel, n),
        out_shape=(pltpu.VMEM((block, width), f32), pltpu.VMEM((1, width), f32)),
        in_specs=[pl.BlockSpec(memory_space=pl.ANY)],
        out_specs=[pl.BlockSpec(memory_space=pltpu.VMEM)] * 2,
        scratch_shapes=[
            pltpu.VMEM((rows, width), f32),
            pltpu.VMEM((rows, width), f32),
            pltpu.VMEM((rows, 2 * width + width // 2), bf16),
            pltpu.VMEM((rows, 2 * width + width // 2), bf16),
            pltpu.VMEM((tasks, 2, block, wide), f32),
            pltpu.VMEM((tasks, 2, block, wide), f32),
            pltpu.VMEM((tasks, 2, block, wide), f32),
            pltpu.VMEM((tasks, block, wide), f32),
            pltpu.VMEM((tasks, block, wide), f32),
            pltpu.VMEM((tasks, block, wide), f32),
            pltpu.VMEM((2, 3, block, wide), f32),
            pltpu.VMEM((3, block, block), f32),
            pltpu.VMEM((half // 2, block, block), f32),
            pltpu.VMEM((half // 2, block, block), f32),
            pltpu.VMEM((n, 1, width), f32),
            pltpu.VMEM((n, 1, width), f32),
            pltpu.VMEM((1, width), f32),
            pltpu.VMEM((n, 2 * width + width // 2), f32),
            dma((LOADS,)),
            dma((LOADS,)), dma((LOADS,)),
            dma, dma,
            dma((tasks, 2)), dma((tasks, 2)),
            dma((tasks,)), dma((tasks,)),
            dma((tasks,)), dma((2, 3)),
            dma((2,)), dma((3,)),
            dma((half // 2,)), dma((half // 2,)),
            dma((n,)), dma((n,)),
            dma, dma,
        ],
        compiler_params=pltpu.CompilerParams(
            collective_id=0, has_side_effects=True, vmem_limit_bytes=60 * 1024 * 1024
        ),
    )(scenario_pnl)
    return covariance, factor_means.reshape(width)


def solution(mesh):
    n, cores = mesh.shape["scen"], mesh.shape["fac"]

    def body(scenario_pnl):
        rows, width = scenario_pnl.shape
        fits = cores == 2 and n % 16 == 0 and n // 4 == 4 and width % (n * 64) == 0
        if fits and rows % (LOADS * TILE) == 0:
            return by_kernel(n, scenario_pnl)
        return on_device(scenario_pnl)

    return jax.shard_map(
        body,
        mesh=mesh,
        in_specs=(P("scen", "fac"),),
        out_specs=(P("scen", "fac"), P("fac")),
        check_vma=False,
    )
```

```python
import functools

import jax
import jax.numpy as jnp
from jax import lax
from jax.experimental import pallas as pl
from jax.experimental.pallas import tpu as pltpu
from jax.sharding import PartitionSpec as P

MESH = pl.DeviceIdType.MESH
LOADS = 4
TILE = 64
AHEAD = 2


def block_gram(left, right):
    return lax.dot_general(
        left,
        right,
        (((0,), (0,)), ((), ())),
        precision=lax.Precision.HIGHEST,
        preferred_element_type=jnp.float32,
    )


def on_device(scenario_pnl):
    rows_here = scenario_pnl.shape[0]
    total_rows = rows_here * lax.axis_size("scen")
    local_sums = jnp.sum(scenario_pnl, axis=0)
    total_sums = lax.psum(local_sums, "scen")
    factor_means = total_sums / total_rows
    local_means = local_sums / rows_here
    data = scenario_pnl - local_means[None, :]
    partial_value = block_gram(lax.all_gather(data, "fac", axis=1, tiled=True), data)
    owned = lax.psum_scatter(partial_value, "scen", scatter_dimension=0, tiled=True)
    gathered = lax.all_gather(local_means, ("scen", "fac"), axis=0, tiled=True)
    spread_rows = gathered.reshape(lax.axis_size("scen"), -1)
    deviations = spread_rows - jnp.mean(spread_rows, axis=0, keepdims=True)
    owned_rows = owned.shape[0]
    column_width = owned.shape[1]
    row_part = lax.dynamic_slice_in_dim(
        deviations, lax.axis_index("scen") * owned_rows, owned_rows, 1
    )
    column_part = lax.dynamic_slice_in_dim(
        deviations, lax.axis_index("fac") * column_width, column_width, 1
    )
    owned = owned + rows_here * block_gram(row_part, column_part)
    covariance = owned / (total_rows - 1)
    return (covariance, factor_means)


def kernel(
    n, x_hbm, cov_ref, mean_ref,
    x_vm, other, hi, lo,
    send1, keep1, recv1, send2, recv2, zpair, zland, zsend, zrecv, xrecv, late,
    turned, landed, sums_own, sums_oth, pair_sum, dev_a,
    load_sem, pair_s, pair_r, ps_s, ps_r, s1_s, s1_r, s2_s, s2_r, z_s, z_r, x_s, x_r,
    t_s, t_r, m_s, m_r, mo_s, mo_r,
):
    rows, width = x_hbm.shape
    half = n // 2
    block = width // half
    quads = n // 4
    strip_blocks = half // 2
    wide = AHEAD * block
    rest = (strip_blocks - AHEAD) * block
    extra = 2 * quads
    wrapped = width + width // 2
    total_rows = rows * n

    s = lax.axis_index("scen")
    c = lax.axis_index("fac")
    z, y, x = s // 4, (s // 2) % 2, s % 2
    first = x * (1 - c) + y * c
    second = y * (1 - c) + x * c
    peer1 = s + (1 - 2 * x) * (1 - c) + (2 - 4 * y) * c
    peer2 = s + (2 - 4 * y) * (1 - c) + (1 - 2 * x) * c
    odd, high, own_z = z % 2, z // 2, 1 - (z // 2 - c) * (z // 2 - c)
    inner, twin = odd + high - 2 * odd * high, z + 1 - 2 * odd

    barrier = pltpu.get_barrier_semaphore()
    me = s * 2 + c

    part = rows // LOADS
    loads = []
    for i in range(LOADS):
        at = pl.ds(i * part, part)
        load = pltpu.make_async_copy(x_hbm.at[at], x_vm.at[at], load_sem.at[i])
        load.start()
        loads.append(load)

    for d in range(1, 2 * n):
        p = (me + d) % (2 * n)
        pl.semaphore_signal(barrier, inc=1, device_id=(p // 2, p % 2), device_id_type=MESH)

    def sums_of(ref, start, count, acc):
        def add(i, acc):
            at = pl.multiple_of(start + i * TILE, TILE)
            return acc + jnp.sum(ref[pl.ds(at, TILE), :].reshape(TILE // 8, 8, width), axis=0)

        return lax.fori_loop(0, count // TILE, add, acc)

    acc = jnp.zeros((8, width), jnp.float32)
    for i in range(LOADS):
        loads[i].wait()
        acc = sums_of(x_vm, i * part, part, acc)
    local_sum = jnp.sum(acc, axis=0, keepdims=True)
    sums_own[s] = local_sum
    mid = width // 2

    def split(ref, mean, cols, base, start, count, wrap):
        def body(i, carry):
            at = pl.ds(pl.multiple_of(start + i * TILE, TILE), TILE)
            data = ref[at, cols] - mean
            top = data.astype(jnp.bfloat16)
            low = (data - top.astype(jnp.float32)).astype(jnp.bfloat16)
            to = pl.ds(pl.multiple_of(base, block), data.shape[1])
            hi[at, to] = top
            lo[at, to] = low
            if wrap:
                hi[at, width:wrapped] = top[:, :mid]
                lo[at, width:wrapped] = low[:, :mid]
            return carry

        lax.fori_loop(0, count // TILE, body, 0)

    split(x_vm, local_sum / rows, slice(None), 0, 0, rows, True)

    def gram(left, right):
        return lax.dot_general(
            left, right, (((0,), (0,)), ((), ())), preferred_element_type=jnp.float32
        )

    def slot_of(k):
        mine = (z + 1 - 2 * odd, 3 - 3 * c, 2 - c, z)[k]
        other_half = (3 * c, 1 + c, z + 1 - 2 * odd, z)[k]
        return own_z * mine + (1 - own_z) * other_half

    def slot_late(t):
        across = 2 * (1 - high)
        return (across + 1 - high, across + high, twin, z)[t - quads]

    def slot(t):
        return slot_of(t) if t < quads else slot_late(t)

    def width_of(t):
        return (wide, rest, block)[t // quads]

    def strip(to, px, py):
        r = (to * 4 + py * 2 + px) % half
        own = 1 - (to // 2 - c) * (to // 2 - c)
        return r + (1 - own) * (wrapped // block), r + (1 - own) * c

    def lanes(start, count):
        return pl.ds(pl.multiple_of(start * block, block), count)

    def product(left, right, count):
        rows_at, cols_at = lanes(left, block), lanes(right, count)
        lh, ll = hi[:, rows_at], lo[:, rows_at]
        rh, rl = hi[:, cols_at], lo[:, cols_at]
        return gram(lh, rh) + (gram(lh, rl) + gram(ll, rh))

    def compute(t, side, dst, send=False):
        def body(j, carry):
            b = (1 - second) + j * (2 * second - 1)
            px, py = side * (1 - c) + b * c, b * (1 - c) + side * c
            if t == extra:
                r = py * 2 + px
                late[quads, 0 if send else 1, j, :, :block] = product(r, r + half // 2, block)
            else:
                to = slot_of(t)
                value = product(*strip(to, px, py), wide + rest)
                dst[t, j] = value[:, :wide]
                late[to, 0 if send else 1, j] = value[:, wide:]
            if send:
                stage1(t, j).start()
            return carry

        lax.fori_loop(0, 2, body, 0)

    def remote(src, dst, send, recv, scen, fac):
        return pltpu.make_async_remote_copy(
            src_ref=src, dst_ref=dst, send_sem=send, recv_sem=recv,
            device_id=(scen, fac), device_id_type=MESH,
        )

    def sent(t, j):
        if t < quads:
            return send1.at[t, j]
        return late.at[quads if t == extra else slot_late(t), 0, j, :, :width_of(t)]

    def kept(t, j):
        if t < quads:
            return keep1[t, j]
        return late[quads if t == extra else slot_late(t), 1, j, :, :width_of(t)]

    def stage1(t, j):
        return remote(
            sent(t, j), recv1.at[t, j, :, :width_of(t)], s1_s.at[t // quads // 2], s1_r.at[t, j], peer1, c
        )

    def stage2(t):
        w = width_of(t)
        return remote(send2.at[t, :, :w], recv2.at[t, :, :w], s2_s.at[t // quads // 2], s2_r.at[t], peer2, c)

    def crosses(t):
        if t >= quads:
            return (1, 1, 0)[t - quads], t - quads
        return (1 - own_z, 1, own_z)[t], t - own_z

    def stage3(t):
        w = width_of(t)
        cross, order = crosses(t)
        last = cross * inner
        place = last + cross * (1 - inner) * (2 + order)
        if t < quads:
            src, dst = zpair.at[t], zland.at[place]
        else:
            src, dst = zsend.at[t, :, :w], zrecv.at[place]
        return remote(
            src, dst, z_s.at[t // quads], z_r.at[t // quads, place],
            (last * slot(t) + (1 - last) * twin) * 4 + y * 2 + x, c,
        )

    def from_z(t, place):
        p = t // quads
        to = zrecv.at[place] if p else zland.at[place]
        remote(to, to, z_s.at[p], z_r.at[p, place], s, 1 - c).wait_recv()
        return to[...]

    def relay3(t):
        cross, order = crosses(t)

        @pl.when(cross * inner == 1)
        def _():
            if t < quads:
                zpair[t] = zpair[t] + from_z(t, 2 + order)
            else:
                zsend[t, :, :rest] = zsend[t, :, :rest] + from_z(t, 2 + order)
            stage3(t).start()

    def stage3_extra(e):
        to = 2 * c + e
        place = (z - to + quads - 1) % quads
        return remote(
            zsend.at[extra, :, :block], xrecv.at[place], x_s.at[e], x_r.at[place],
            to * 4 + y * 2 + x, c,
        )

    def with_stage3(t, act, every=False):
        if t == extra:
            for e in range(2):
                pl.when(2 * c + e != z)(act(stage3_extra(e)))
        elif t % quads < quads - 1:
            pl.when((crosses(t)[0] * inner == 0) | every)(act(stage3(t)))

    def relay1(t):
        w = width_of(t)
        if t < quads:
            for j in range(2):
                stage1(t, j).wait_recv()
                zpair[t, j] = keep1[t, j] + recv1[t, j, :, :w]
            if t:
                with_stage3(t, lambda copy: copy.start)
            else:
                pl.when((own_z == 0) & (inner == 0))(stage3(0).start)
            if t == 2:
                pl.when(own_z == 1)(stage3(0).start)
            return
        stage1(t, 0).wait_recv()
        send2[t, :, :w] = kept(t, 0) + recv1[t, 0, :, :w]
        stage2(t).start()

    def join1():
        t = quads - 1
        a, b = from_z(t, 0), from_z(t, 1)
        send2[t, :, :wide] = zpair[t, 0] + a[0] + b[0]
        stage2(t).start()
        zsend[t, :, :wide] = zpair[t, 1] + a[1] + b[1]

    def relay2(t):
        w = width_of(t)
        stage1(t, 1).wait_recv()
        stage2(t).wait_recv()
        zsend[t, :, :w] = kept(t, 1) + recv1[t, 1, :, :w] + recv2[t, :, :w]
        with_stage3(t, lambda copy: copy.start)

    def send_stage(t):
        for j in range(2):
            stage1(t, j).start()

    def pair_copy(i, mine):
        h = own_z * (1 - odd) + (1 - own_z) * c if mine else own_z * (1 - c) + (1 - own_z) * (1 - odd)
        h = h if i < 2 else 1 - h
        at = pl.ds(i % 2 * (rows // 2), rows // 2), pl.ds(pl.multiple_of(h * mid, block), mid)
        return h, remote(x_vm.at[at], other.at[at], pair_s, pair_r.at[i // 2], s, 1 - c)

    def pair_part(half_at):
        h, _ = pair_copy(2 * half_at, False)
        cols = pl.ds(pl.multiple_of(h * mid, block), mid)
        to = other.at[:, cols]
        remote(to, to, pair_s, pair_r.at[half_at], s, 1 - c).wait_recv()
        split(other, pair_sum[:, cols] / rows, cols, wrapped + h * mid, 0, rows, False)

    def mean_copy(d):
        p = (s + d) % n
        return remote(sums_own.at[s], sums_own.at[s], m_s, m_r, p, c)

    pl.semaphore_wait(barrier, 2 * n - 1)
    pair_mean = remote(sums_own.at[s], pair_sum, ps_s, ps_r, s, 1 - c)
    pair_mean.start()
    for i in range(4):
        pair_copy(i, True)[1].start()
    compute(extra, 1 - first, send1, True)
    compute(0, 1 - first, send1, True)
    for d in range(1, n):
        mean_copy(d).start()
    compute(extra, first, keep1)
    compute(0, first, keep1)
    relay1(extra)

    pair_mean.wait_recv()
    pair_part(0)
    compute(1, 1 - first, send1, True)
    compute(1, first, keep1)
    relay1(0)
    pair_part(1)
    compute(2, 1 - first, send1, True)
    relay2(extra)
    compute(2, first, keep1)
    compute(3, 1 - first, send1, True)
    for t in range(quads, 2 * quads):
        send_stage(t)
    relay1(1)
    compute(3, first, keep1)
    relay1(2)
    relay3(0)
    relay1(3)
    relay1(quads)
    most_sums = sums_own.at[pl.ds(0, n - 1)]
    all_means = remote(most_sums, most_sums, m_s, m_r, s, 1 - c)
    all_means.wait_recv()
    swap = remote(sums_own, sums_oth, mo_s, mo_r, s, 1 - c)
    swap.start()
    relay3(1)

    def deviations(ref):
        sums = ref[...].reshape(n, width)
        total = jnp.sum(sums, axis=0, keepdims=True)
        return sums / rows - total / total_rows, total / total_rows

    dev, means = deviations(sums_own)
    mean_ref[...] = means
    dev_a[:, :width] = dev
    dev_a[:, width:wrapped] = dev[:, :mid]
    swap.wait_recv()
    dev_a[:, wrapped:] = deviations(sums_oth)[0]

    r = s % half
    start = r + (1 - own_z) * c

    def put(q, value):
        cov_ref[:, lanes(q % half, block)] = value

    def turn_copy(d):
        return remote(
            turned.at[d], landed.at[d], t_s.at[(d + strip_blocks - 1) // strip_blocks], t_r.at[d],
            c * half + (start + d) % half, own_z * c + (1 - own_z) * (1 - c),
        )

    def mirrored(d, act):
        if d:
            act()
        else:
            pl.when(own_z == 0)(act)

    def finish(p):
        t = p * quads + quads - 1
        w = width_of(t)
        if p:
            arrived = [from_z(t, place) for place in range(2)]
        else:
            stage2(t).wait_recv()
            arrived = [recv2[t, :, :w]]
        left, right = strip(z, x, y)
        right = right + p * AHEAD
        shift = block_gram(dev_a[:, lanes(left, block)], dev_a[:, lanes(right, w)])
        value = zsend[t, :, :w]
        for other_z in arrived:
            value = value + other_z
        value = (value + rows * shift) / (total_rows - 1)
        pieces = piece(p)
        for i, d in enumerate(pieces):
            turned[d] = value[:, i * block:(i + 1) * block].T
            mirrored(d, turn_copy(d).start)
        for i, d in enumerate(pieces):
            put(start + d, value[:, i * block:(i + 1) * block])

    def piece(p):
        return range(AHEAD, strip_blocks) if p else range(AHEAD)

    def land(p):
        for d in piece(p):
            def arrive():
                turn_copy(d).wait_recv()
                put(r - (1 - own_z) * (1 - c) - d + 2 * half, landed[d])

            mirrored(d, arrive)

    def finish_extra():
        @pl.when(own_z == 1)
        def _():
            for place in range(quads - 1):
                remote(
                    zsend.at[extra, :, :block], xrecv.at[place], x_s.at[0], x_r.at[place], s, 1 - c
                ).wait_recv()
            left = y * 2 + x
            shift = block_gram(
                dev_a[:, lanes(left, block)], dev_a[:, lanes(left + half // 2, block)]
            )
            value = zsend[extra, :, :block]
            for place in range(quads - 1):
                value = value + xrecv[place]
            value = (value + rows * shift) / (total_rows - 1)

            @pl.when(odd == 0)
            def _():
                put(r + half // 2, value)

            @pl.when(odd == 1)
            def _():
                put(r + half // 2, value.T)

    relay1(quads + 1)
    relay2(quads)
    relay3(2)
    relay1(quads + 2)
    relay2(quads + 1)
    relay3(quads)
    join1()
    relay1(quads + 3)
    relay2(quads + 2)
    relay3(quads + 1)
    finish(0)
    finish_extra()
    relay2(quads + 3)
    finish(1)
    land(0)
    land(1)

    def sent_bytes(ref, sem):
        remote(ref, ref, sem, ps_r, s, 1 - c).wait_send()

    pair_mean.wait_send()
    swap.wait_send()
    sent_bytes(other, pair_s)
    all_means.wait_send()
    for d in range(min(2, strip_blocks)):
        pl.when((d == 1) | (own_z == 0))(
            functools.partial(
                sent_bytes, landed.at[pl.ds(d, (1, strip_blocks - 1)[d])], t_s.at[d]
            )
        )
    sent_bytes(send1, s1_s.at[0])
    sent_bytes(late.at[pl.ds(0, quads), 1], s1_s.at[0])
    sent_bytes(late.at[quads, 1, :, :, :block], s1_s.at[1])
    sent_bytes(recv2.at[quads - 1, :, :wide], s2_s.at[0])
    sent_bytes(recv2.at[pl.ds(quads, quads), :, :rest], s2_s.at[0])
    sent_bytes(recv2.at[extra, :, :block], s2_s.at[1])
    sent_bytes(zpair.at[pl.ds(0, quads - 1)], z_s.at[0])
    sent_bytes(zsend.at[pl.ds(quads, quads - 1), :, :rest], z_s.at[1])
    with_stage3(extra, lambda copy: copy.wait_send)


def by_kernel(n, scenario_pnl):
    rows, width = scenario_pnl.shape
    half = n // 2
    block = width // half
    wide, rest = AHEAD * block, (half // 2 - AHEAD) * block
    most = max(wide, rest)
    tasks = 2 * (n // 4) + 1
    f32, bf16 = jnp.float32, jnp.bfloat16
    dma = pltpu.SemaphoreType.DMA
    covariance, factor_means = pl.pallas_call(
        functools.partial(kernel, n),
        out_shape=(pltpu.VMEM((block, width), f32), pltpu.VMEM((1, width), f32)),
        in_specs=[pl.BlockSpec(memory_space=pl.ANY)],
        out_specs=[pl.BlockSpec(memory_space=pltpu.VMEM)] * 2,
        scratch_shapes=[
            pltpu.VMEM((rows, width), f32),
            pltpu.VMEM((rows, width), f32),
            pltpu.VMEM((rows, 2 * width + width // 2), bf16),
            pltpu.VMEM((rows, 2 * width + width // 2), bf16),
            pltpu.VMEM((n // 4, 2, block, wide), f32),
            pltpu.VMEM((n // 4, 2, block, wide), f32),
            pltpu.VMEM((tasks, 2, block, most), f32),
            pltpu.VMEM((tasks, block, most), f32),
            pltpu.VMEM((tasks, block, most), f32),
            pltpu.VMEM((n // 4, 2, block, wide), f32),
            pltpu.VMEM((4, 2, block, wide), f32),
            pltpu.VMEM((tasks, block, most), f32),
            pltpu.VMEM((4, block, rest), f32),
            pltpu.VMEM((3, block, block), f32),
            pltpu.VMEM((n // 4 + 1, 2, 2, block, rest), f32),
            pltpu.VMEM((half // 2, block, block), f32),
            pltpu.VMEM((half // 2, block, block), f32),
            pltpu.VMEM((n, 1, width), f32),
            pltpu.VMEM((n, 1, width), f32),
            pltpu.VMEM((1, width), f32),
            pltpu.VMEM((n, 2 * width + width // 2), f32),
            dma((LOADS,)),
            dma, dma((2,)),
            dma, dma,
            dma((2,)), dma((tasks, 2)),
            dma((2,)), dma((tasks,)),
            dma((2,)), dma((2, 4)),
            dma((2,)), dma((3,)),
            dma((2,)), dma((half // 2,)),
            dma, dma,
            dma, dma,
        ],
        compiler_params=pltpu.CompilerParams(
            collective_id=0, has_side_effects=True, vmem_limit_bytes=60 * 1024 * 1024
        ),
    )(scenario_pnl)
    return covariance, factor_means.reshape(width)


def solution(mesh):
    n, cores = mesh.shape["scen"], mesh.shape["fac"]

    def body(scenario_pnl):
        rows, width = scenario_pnl.shape
        fits = cores == 2 and n % 16 == 0 and n // 4 == 4 and width % (n * 64) == 0
        if fits and rows % (LOADS * TILE) == 0:
            return by_kernel(n, scenario_pnl)
        return on_device(scenario_pnl)

    return jax.shard_map(
        body,
        mesh=mesh,
        in_specs=(P("scen", "fac"),),
        out_specs=(P("scen", "fac"), P("fac")),
        check_vma=False,
    )
```

```python
import functools

import jax
import jax.numpy as jnp
from jax import lax
from jax.experimental import pallas as pl
from jax.experimental.pallas import tpu as pltpu
from jax.sharding import PartitionSpec as P

MESH = pl.DeviceIdType.MESH
LOADS = 4
TILE = 64
AHEAD = 2


def block_gram(left, right):
    return lax.dot_general(
        left,
        right,
        (((0,), (0,)), ((), ())),
        precision=lax.Precision.HIGHEST,
        preferred_element_type=jnp.float32,
    )


def on_device(scenario_pnl):
    rows_here = scenario_pnl.shape[0]
    total_rows = rows_here * lax.axis_size("scen")
    local_sums = jnp.sum(scenario_pnl, axis=0)
    total_sums = lax.psum(local_sums, "scen")
    factor_means = total_sums / total_rows
    local_means = local_sums / rows_here
    data = scenario_pnl - local_means[None, :]
    partial_value = block_gram(lax.all_gather(data, "fac", axis=1, tiled=True), data)
    owned = lax.psum_scatter(partial_value, "scen", scatter_dimension=0, tiled=True)
    gathered = lax.all_gather(local_means, ("scen", "fac"), axis=0, tiled=True)
    spread_rows = gathered.reshape(lax.axis_size("scen"), -1)
    deviations = spread_rows - jnp.mean(spread_rows, axis=0, keepdims=True)
    owned_rows = owned.shape[0]
    column_width = owned.shape[1]
    row_part = lax.dynamic_slice_in_dim(
        deviations, lax.axis_index("scen") * owned_rows, owned_rows, 1
    )
    column_part = lax.dynamic_slice_in_dim(
        deviations, lax.axis_index("fac") * column_width, column_width, 1
    )
    owned = owned + rows_here * block_gram(row_part, column_part)
    covariance = owned / (total_rows - 1)
    return (covariance, factor_means)


def kernel(
    n, x_hbm, cov_ref, mean_ref,
    x_vm, other, hi, lo,
    send1, keep1, recv1, send2, recv2, zpair, zland, zsend, zrecv, xrecv, late,
    turned, landed, sums_own, sums_oth, pair_sum, dev_a,
    load_sem, pair_s, pair_r, ps_s, ps_r, s1_s, s1_r, s2_s, s2_r, z_s, z_r, x_s, x_r,
    t_s, t_r, m_s, m_r, mo_s, mo_r,
):
    rows, width = x_hbm.shape
    half = n // 2
    block = width // half
    quads = n // 4
    strip_blocks = half // 2
    wide = AHEAD * block
    rest = (strip_blocks - AHEAD) * block
    extra = 2 * quads
    wrapped = width + width // 2
    total_rows = rows * n

    s = lax.axis_index("scen")
    c = lax.axis_index("fac")
    z, y, x = s // 4, (s // 2) % 2, s % 2
    first = x * (1 - c) + y * c
    second = y * (1 - c) + x * c
    peer1 = s + (1 - 2 * x) * (1 - c) + (2 - 4 * y) * c
    peer2 = s + (2 - 4 * y) * (1 - c) + (1 - 2 * x) * c
    odd, high, own_z = z % 2, z // 2, 1 - (z // 2 - c) * (z // 2 - c)
    inner, twin = odd + high - 2 * odd * high, z + 1 - 2 * odd

    barrier = pltpu.get_barrier_semaphore()
    me = s * 2 + c

    part = rows // LOADS
    loads = []
    for i in range(LOADS):
        at = pl.ds(i * part, part)
        load = pltpu.make_async_copy(x_hbm.at[at], x_vm.at[at], load_sem.at[i])
        load.start()
        loads.append(load)

    for d in range(1, 2 * n):
        p = (me + d) % (2 * n)
        pl.semaphore_signal(barrier, inc=1, device_id=(p // 2, p % 2), device_id_type=MESH)

    def sums_of(ref, start, count, acc):
        def add(i, acc):
            at = pl.multiple_of(start + i * TILE, TILE)
            return acc + jnp.sum(ref[pl.ds(at, TILE), :].reshape(TILE // 8, 8, width), axis=0)

        return lax.fori_loop(0, count // TILE, add, acc)

    acc = jnp.zeros((8, width), jnp.float32)
    for i in range(LOADS):
        loads[i].wait()
        acc = sums_of(x_vm, i * part, part, acc)
    local_sum = jnp.sum(acc, axis=0, keepdims=True)
    sums_own[s] = local_sum
    mid = width // 2

    def split(ref, mean, cols, base, start, count, wrap):
        def body(i, carry):
            at = pl.ds(pl.multiple_of(start + i * TILE, TILE), TILE)
            data = ref[at, cols] - mean
            top = data.astype(jnp.bfloat16)
            low = (data - top.astype(jnp.float32)).astype(jnp.bfloat16)
            to = pl.ds(pl.multiple_of(base, block), data.shape[1])
            hi[at, to] = top
            lo[at, to] = low
            if wrap:
                hi[at, width:wrapped] = top[:, :mid]
                lo[at, width:wrapped] = low[:, :mid]
            return carry

        lax.fori_loop(0, count // TILE, body, 0)

    split(x_vm, local_sum / rows, slice(None), 0, 0, rows, True)

    def gram(left, right):
        return lax.dot_general(
            left, right, (((0,), (0,)), ((), ())), preferred_element_type=jnp.float32
        )

    def slot_of(k):
        mine = (z + 1 - 2 * odd, 3 - 3 * c, 2 - c, z)[k]
        other_half = (3 * c, 1 + c, z + 1 - 2 * odd, z)[k]
        return own_z * mine + (1 - own_z) * other_half

    def slot_late(t):
        across = 2 * (1 - high)
        return (across + 1 - high, across + high, twin, z)[t - quads]

    def slot(t):
        return slot_of(t) if t < quads else slot_late(t)

    def width_of(t):
        return (wide, rest, block)[t // quads]

    def strip(to, px, py):
        r = (to * 4 + py * 2 + px) % half
        own = 1 - (to // 2 - c) * (to // 2 - c)
        return r + (1 - own) * (wrapped // block), r + (1 - own) * c

    def lanes(start, count):
        return pl.ds(pl.multiple_of(start * block, block), count)

    def product(left, right, count):
        rows_at, cols_at = lanes(left, block), lanes(right, count)
        lh, ll = hi[:, rows_at], lo[:, rows_at]
        rh, rl = hi[:, cols_at], lo[:, cols_at]
        return gram(lh, rh) + (gram(lh, rl) + gram(ll, rh))

    def compute(t, side, dst, send=False):
        def body(j, carry):
            b = (1 - second) + j * (2 * second - 1)
            px, py = side * (1 - c) + b * c, b * (1 - c) + side * c
            if t == extra:
                r = py * 2 + px
                late[quads, 0 if send else 1, j, :, :block] = product(r, r + half // 2, block)
            else:
                to = slot_of(t)
                value = product(*strip(to, px, py), wide + rest)
                dst[t, j] = value[:, :wide]
                late[to, 0 if send else 1, j] = value[:, wide:]
            if send:
                stage1(t, j).start()
            return carry

        lax.fori_loop(0, 2, body, 0)

    def remote(src, dst, send, recv, scen, fac):
        return pltpu.make_async_remote_copy(
            src_ref=src, dst_ref=dst, send_sem=send, recv_sem=recv,
            device_id=(scen, fac), device_id_type=MESH,
        )

    def sent(t, j):
        if t < quads:
            return send1.at[t, j]
        return late.at[quads if t == extra else slot_late(t), 0, j, :, :width_of(t)]

    def kept(t, j):
        if t < quads:
            return keep1[t, j]
        return late[quads if t == extra else slot_late(t), 1, j, :, :width_of(t)]

    def stage1(t, j):
        return remote(
            sent(t, j), recv1.at[t, j, :, :width_of(t)], s1_s.at[t // quads // 2], s1_r.at[t, j], peer1, c
        )

    def stage2(t):
        w = width_of(t)
        return remote(send2.at[t, :, :w], recv2.at[t, :, :w], s2_s.at[t // quads // 2], s2_r.at[t], peer2, c)

    def crosses(t):
        if t >= quads:
            return (1, 1, 0)[t - quads], t - quads
        return (1 - own_z, 1, own_z)[t], t - own_z

    def stage3(t):
        w = width_of(t)
        cross, order = crosses(t)
        last = cross * inner
        place = last + cross * (1 - inner) * (2 + order)
        if t < quads:
            src, dst = zpair.at[t], zland.at[place]
        else:
            src, dst = zsend.at[t, :, :w], zrecv.at[place]
        return remote(
            src, dst, z_s.at[t // quads], z_r.at[t // quads, place],
            (last * slot(t) + (1 - last) * twin) * 4 + y * 2 + x, c,
        )

    def from_z(t, place):
        p = t // quads
        to = zrecv.at[place] if p else zland.at[place]
        remote(to, to, z_s.at[p], z_r.at[p, place], s, 1 - c).wait_recv()
        return to[...]

    def relay3(t):
        cross, order = crosses(t)

        @pl.when(cross * inner == 1)
        def _():
            if t < quads:
                zpair[t] = zpair[t] + from_z(t, 2 + order)
            else:
                zsend[t, :, :rest] = zsend[t, :, :rest] + from_z(t, 2 + order)
            stage3(t).start()

    def stage3_extra(e):
        to = 2 * c + e
        place = (z - to + quads - 1) % quads
        return remote(
            zsend.at[extra, :, :block], xrecv.at[place], x_s.at[e], x_r.at[place],
            to * 4 + y * 2 + x, c,
        )

    def with_stage3(t, act, every=False):
        if t == extra:
            for e in range(2):
                pl.when(2 * c + e != z)(act(stage3_extra(e)))
        elif t % quads < quads - 1:
            pl.when((crosses(t)[0] * inner == 0) | every)(act(stage3(t)))

    def relay1(t):
        w = width_of(t)
        if t < quads:
            for j in range(2):
                stage1(t, j).wait_recv()
                zpair[t, j] = keep1[t, j] + recv1[t, j, :, :w]
            if t:
                with_stage3(t, lambda copy: copy.start)
            else:
                pl.when((own_z == 0) & (inner == 0))(stage3(0).start)
            if t == 2:
                pl.when(own_z == 1)(stage3(0).start)
            return
        stage1(t, 0).wait_recv()
        send2[t, :, :w] = kept(t, 0) + recv1[t, 0, :, :w]
        stage2(t).start()

    def join1():
        t = quads - 1
        a, b = from_z(t, 0), from_z(t, 1)
        send2[t, :, :wide] = zpair[t, 0] + a[0] + b[0]
        stage2(t).start()
        zsend[t, :, :wide] = zpair[t, 1] + a[1] + b[1]

    def relay2(t):
        w = width_of(t)
        stage1(t, 1).wait_recv()
        stage2(t).wait_recv()
        zsend[t, :, :w] = kept(t, 1) + recv1[t, 1, :, :w] + recv2[t, :, :w]
        with_stage3(t, lambda copy: copy.start)

    def send_stage(t):
        for j in range(2):
            stage1(t, j).start()

    def pair_copy(i, mine):
        h = own_z * (1 - odd) + (1 - own_z) * c if mine else own_z * (1 - c) + (1 - own_z) * (1 - odd)
        h = h if i < 2 else 1 - h
        at = pl.ds(i % 2 * (rows // 2), rows // 2), pl.ds(pl.multiple_of(h * mid, block), mid)
        return h, remote(x_vm.at[at], other.at[at], pair_s, pair_r.at[i // 2], s, 1 - c)

    def pair_part(half_at):
        h, _ = pair_copy(2 * half_at, False)
        cols = pl.ds(pl.multiple_of(h * mid, block), mid)
        to = other.at[:, cols]
        remote(to, to, pair_s, pair_r.at[half_at], s, 1 - c).wait_recv()
        split(other, pair_sum[:, cols] / rows, cols, wrapped + h * mid, 0, rows, False)

    def mean_copy(d):
        p = (s + d) % n
        return remote(sums_own.at[s], sums_own.at[s], m_s, m_r, p, c)

    pl.semaphore_wait(barrier, 2 * n - 1)
    pair_mean = remote(sums_own.at[s], pair_sum, ps_s, ps_r, s, 1 - c)
    pair_mean.start()
    for i in range(4):
        pair_copy(i, True)[1].start()
    compute(extra, 1 - first, send1, True)
    compute(0, 1 - first, send1, True)
    for d in range(1, n):
        mean_copy(d).start()
    compute(extra, first, keep1)
    compute(0, first, keep1)
    relay1(extra)

    pair_mean.wait_recv()
    pair_part(0)
    compute(1, 1 - first, send1, True)
    compute(1, first, keep1)
    relay1(0)
    relay2(extra)
    pair_part(1)
    compute(2, 1 - first, send1, True)
    compute(2, first, keep1)
    compute(3, 1 - first, send1, True)
    for t in range(quads, 2 * quads):
        send_stage(t)
    relay1(1)
    compute(3, first, keep1)
    relay1(2)
    relay3(0)
    relay1(3)
    relay1(quads)
    most_sums = sums_own.at[pl.ds(0, n - 1)]
    all_means = remote(most_sums, most_sums, m_s, m_r, s, 1 - c)
    all_means.wait_recv()
    swap = remote(sums_own, sums_oth, mo_s, mo_r, s, 1 - c)
    swap.start()
    relay3(1)

    def deviations(ref):
        sums = ref[...].reshape(n, width)
        total = jnp.sum(sums, axis=0, keepdims=True)
        return sums / rows - total / total_rows, total / total_rows

    dev, means = deviations(sums_own)
    mean_ref[...] = means
    dev_a[:, :width] = dev
    dev_a[:, width:wrapped] = dev[:, :mid]
    swap.wait_recv()
    dev_a[:, wrapped:] = deviations(sums_oth)[0]

    r = s % half
    start = r + (1 - own_z) * c

    def put(q, value):
        cov_ref[:, lanes(q % half, block)] = value

    def turn_copy(d):
        return remote(
            turned.at[d], landed.at[d], t_s.at[(d + strip_blocks - 1) // strip_blocks], t_r.at[d],
            c * half + (start + d) % half, own_z * c + (1 - own_z) * (1 - c),
        )

    def mirrored(d, act):
        if d:
            act()
        else:
            pl.when(own_z == 0)(act)

    def finish(p):
        t = p * quads + quads - 1
        w = width_of(t)
        if p:
            arrived = [from_z(t, place) for place in range(2)]
        else:
            stage2(t).wait_recv()
            arrived = [recv2[t, :, :w]]
        left, right = strip(z, x, y)
        right = right + p * AHEAD
        shift = block_gram(dev_a[:, lanes(left, block)], dev_a[:, lanes(right, w)])
        value = zsend[t, :, :w]
        for other_z in arrived:
            value = value + other_z
        value = (value + rows * shift) / (total_rows - 1)
        pieces = piece(p)
        for i, d in enumerate(pieces):
            turned[d] = value[:, i * block:(i + 1) * block].T
            mirrored(d, turn_copy(d).start)
        for i, d in enumerate(pieces):
            put(start + d, value[:, i * block:(i + 1) * block])

    def piece(p):
        return range(AHEAD, strip_blocks) if p else range(AHEAD)

    def land(p):
        for d in piece(p):
            def arrive():
                turn_copy(d).wait_recv()
                put(r - (1 - own_z) * (1 - c) - d + 2 * half, landed[d])

            mirrored(d, arrive)

    def finish_extra():
        @pl.when(own_z == 1)
        def _():
            for place in range(quads - 1):
                remote(
                    zsend.at[extra, :, :block], xrecv.at[place], x_s.at[0], x_r.at[place], s, 1 - c
                ).wait_recv()
            left = y * 2 + x
            shift = block_gram(
                dev_a[:, lanes(left, block)], dev_a[:, lanes(left + half // 2, block)]
            )
            value = zsend[extra, :, :block]
            for place in range(quads - 1):
                value = value + xrecv[place]
            value = (value + rows * shift) / (total_rows - 1)

            @pl.when(odd == 0)
            def _():
                put(r + half // 2, value)

            @pl.when(odd == 1)
            def _():
                put(r + half // 2, value.T)

    relay1(quads + 1)
    relay2(quads)
    relay3(2)
    relay1(quads + 2)
    relay2(quads + 1)
    relay3(quads)
    join1()
    relay1(quads + 3)
    relay2(quads + 2)
    relay3(quads + 1)
    finish(0)
    finish_extra()
    relay2(quads + 3)
    finish(1)
    land(0)
    land(1)

    def sent_bytes(ref, sem):
        remote(ref, ref, sem, ps_r, s, 1 - c).wait_send()

    pair_mean.wait_send()
    swap.wait_send()
    sent_bytes(other, pair_s)
    all_means.wait_send()
    for d in range(min(2, strip_blocks)):
        pl.when((d == 1) | (own_z == 0))(
            functools.partial(
                sent_bytes, landed.at[pl.ds(d, (1, strip_blocks - 1)[d])], t_s.at[d]
            )
        )
    sent_bytes(send1, s1_s.at[0])
    sent_bytes(late.at[pl.ds(0, quads), 1], s1_s.at[0])
    sent_bytes(late.at[quads, 1, :, :, :block], s1_s.at[1])
    sent_bytes(recv2.at[quads - 1, :, :wide], s2_s.at[0])
    sent_bytes(recv2.at[pl.ds(quads, quads), :, :rest], s2_s.at[0])
    sent_bytes(recv2.at[extra, :, :block], s2_s.at[1])
    sent_bytes(zpair.at[pl.ds(0, quads - 1)], z_s.at[0])
    sent_bytes(zsend.at[pl.ds(quads, quads - 1), :, :rest], z_s.at[1])
    with_stage3(extra, lambda copy: copy.wait_send)


def by_kernel(n, scenario_pnl):
    rows, width = scenario_pnl.shape
    half = n // 2
    block = width // half
    wide, rest = AHEAD * block, (half // 2 - AHEAD) * block
    most = max(wide, rest)
    tasks = 2 * (n // 4) + 1
    f32, bf16 = jnp.float32, jnp.bfloat16
    dma = pltpu.SemaphoreType.DMA
    covariance, factor_means = pl.pallas_call(
        functools.partial(kernel, n),
        out_shape=(pltpu.VMEM((block, width), f32), pltpu.VMEM((1, width), f32)),
        in_specs=[pl.BlockSpec(memory_space=pl.ANY)],
        out_specs=[pl.BlockSpec(memory_space=pltpu.VMEM)] * 2,
        scratch_shapes=[
            pltpu.VMEM((rows, width), f32),
            pltpu.VMEM((rows, width), f32),
            pltpu.VMEM((rows, 2 * width + width // 2), bf16),
            pltpu.VMEM((rows, 2 * width + width // 2), bf16),
            pltpu.VMEM((n // 4, 2, block, wide), f32),
            pltpu.VMEM((n // 4, 2, block, wide), f32),
            pltpu.VMEM((tasks, 2, block, most), f32),
            pltpu.VMEM((tasks, block, most), f32),
            pltpu.VMEM((tasks, block, most), f32),
            pltpu.VMEM((n // 4, 2, block, wide), f32),
            pltpu.VMEM((4, 2, block, wide), f32),
            pltpu.VMEM((tasks, block, most), f32),
            pltpu.VMEM((4, block, rest), f32),
            pltpu.VMEM((3, block, block), f32),
            pltpu.VMEM((n // 4 + 1, 2, 2, block, rest), f32),
            pltpu.VMEM((half // 2, block, block), f32),
            pltpu.VMEM((half // 2, block, block), f32),
            pltpu.VMEM((n, 1, width), f32),
            pltpu.VMEM((n, 1, width), f32),
            pltpu.VMEM((1, width), f32),
            pltpu.VMEM((n, 2 * width + width // 2), f32),
            dma((LOADS,)),
            dma, dma((2,)),
            dma, dma,
            dma((2,)), dma((tasks, 2)),
            dma((2,)), dma((tasks,)),
            dma((2,)), dma((2, 4)),
            dma((2,)), dma((3,)),
            dma((2,)), dma((half // 2,)),
            dma, dma,
            dma, dma,
        ],
        compiler_params=pltpu.CompilerParams(
            collective_id=0, has_side_effects=True, vmem_limit_bytes=60 * 1024 * 1024
        ),
    )(scenario_pnl)
    return covariance, factor_means.reshape(width)


def solution(mesh):
    n, cores = mesh.shape["scen"], mesh.shape["fac"]

    def body(scenario_pnl):
        rows, width = scenario_pnl.shape
        fits = cores == 2 and n % 16 == 0 and n // 4 == 4 and width % (n * 64) == 0
        if fits and rows % (LOADS * TILE) == 0:
            return by_kernel(n, scenario_pnl)
        return on_device(scenario_pnl)

    return jax.shard_map(
        body,
        mesh=mesh,
        in_specs=(P("scen", "fac"),),
        out_specs=(P("scen", "fac"), P("fac")),
        check_vma=False,
    )
```

```python
import functools

import jax
import jax.numpy as jnp
from jax import lax
from jax.experimental import pallas as pl
from jax.experimental.pallas import tpu as pltpu
from jax.sharding import PartitionSpec as P

MESH = pl.DeviceIdType.MESH
LOADS = 4
TILE = 64
AHEAD = 2


def block_gram(left, right):
    return lax.dot_general(
        left,
        right,
        (((0,), (0,)), ((), ())),
        precision=lax.Precision.HIGHEST,
        preferred_element_type=jnp.float32,
    )


def on_device(scenario_pnl):
    rows_here = scenario_pnl.shape[0]
    total_rows = rows_here * lax.axis_size("scen")
    local_sums = jnp.sum(scenario_pnl, axis=0)
    total_sums = lax.psum(local_sums, "scen")
    factor_means = total_sums / total_rows
    local_means = local_sums / rows_here
    data = scenario_pnl - local_means[None, :]
    partial_value = block_gram(lax.all_gather(data, "fac", axis=1, tiled=True), data)
    owned = lax.psum_scatter(partial_value, "scen", scatter_dimension=0, tiled=True)
    gathered = lax.all_gather(local_means, ("scen", "fac"), axis=0, tiled=True)
    spread_rows = gathered.reshape(lax.axis_size("scen"), -1)
    deviations = spread_rows - jnp.mean(spread_rows, axis=0, keepdims=True)
    owned_rows = owned.shape[0]
    column_width = owned.shape[1]
    row_part = lax.dynamic_slice_in_dim(
        deviations, lax.axis_index("scen") * owned_rows, owned_rows, 1
    )
    column_part = lax.dynamic_slice_in_dim(
        deviations, lax.axis_index("fac") * column_width, column_width, 1
    )
    owned = owned + rows_here * block_gram(row_part, column_part)
    covariance = owned / (total_rows - 1)
    return (covariance, factor_means)


def kernel(
    n, x_hbm, cov_ref, mean_ref,
    x_vm, other, hi, lo,
    send1, keep1, recv1, send2, recv2, zpair, zland, zsend, zrecv, xrecv, late,
    turned, landed, sums_own, sums_oth, pair_sum, dev_a,
    load_sem, pair_s, pair_r, ps_s, ps_r, s1_s, s1_r, s2_s, s2_r, z_s, z_r, x_s, x_r,
    t_s, t_r, m_s, m_r, mo_s, mo_r,
):
    rows, width = x_hbm.shape
    half = n // 2
    block = width // half
    quads = n // 4
    strip_blocks = half // 2
    wide = AHEAD * block
    rest = (strip_blocks - AHEAD) * block
    extra = 2 * quads
    wrapped = width + width // 2
    total_rows = rows * n

    s = lax.axis_index("scen")
    c = lax.axis_index("fac")
    z, y, x = s // 4, (s // 2) % 2, s % 2
    first = x * (1 - c) + y * c
    second = y * (1 - c) + x * c
    peer1 = s + (1 - 2 * x) * (1 - c) + (2 - 4 * y) * c
    peer2 = s + (2 - 4 * y) * (1 - c) + (1 - 2 * x) * c
    odd, high, own_z = z % 2, z // 2, 1 - (z // 2 - c) * (z // 2 - c)
    inner, twin = odd + high - 2 * odd * high, z + 1 - 2 * odd

    barrier = pltpu.get_barrier_semaphore()
    me = s * 2 + c

    part = rows // LOADS
    loads = []
    for i in range(LOADS):
        at = pl.ds(i * part, part)
        load = pltpu.make_async_copy(x_hbm.at[at], x_vm.at[at], load_sem.at[i])
        load.start()
        loads.append(load)

    for d in range(1, 2 * n):
        p = (me + d) % (2 * n)
        pl.semaphore_signal(barrier, inc=1, device_id=(p // 2, p % 2), device_id_type=MESH)

    def sums_of(ref, start, count, acc):
        def add(i, acc):
            at = pl.multiple_of(start + i * TILE, TILE)
            return acc + jnp.sum(ref[pl.ds(at, TILE), :].reshape(TILE // 8, 8, width), axis=0)

        return lax.fori_loop(0, count // TILE, add, acc)

    acc = jnp.zeros((8, width), jnp.float32)
    for i in range(LOADS):
        loads[i].wait()
        acc = sums_of(x_vm, i * part, part, acc)
    local_sum = jnp.sum(acc, axis=0, keepdims=True)
    sums_own[s] = local_sum
    mid = width // 2

    def split(ref, mean, cols, base, start, count, wrap):
        def body(i, carry):
            at = pl.ds(pl.multiple_of(start + i * TILE, TILE), TILE)
            data = ref[at, cols] - mean
            top = data.astype(jnp.bfloat16)
            low = (data - top.astype(jnp.float32)).astype(jnp.bfloat16)
            to = pl.ds(pl.multiple_of(base, block), data.shape[1])
            hi[at, to] = top
            lo[at, to] = low
            if wrap:
                hi[at, width:wrapped] = top[:, :mid]
                lo[at, width:wrapped] = low[:, :mid]
            return carry

        lax.fori_loop(0, count // TILE, body, 0)

    split(x_vm, local_sum / rows, slice(None), 0, 0, rows, True)

    def gram(left, right):
        return lax.dot_general(
            left, right, (((0,), (0,)), ((), ())), preferred_element_type=jnp.float32
        )

    def slot_of(k):
        mine = (z + 1 - 2 * odd, 3 - 3 * c, 2 - c, z)[k]
        other_half = (3 * c, 1 + c, z + 1 - 2 * odd, z)[k]
        return own_z * mine + (1 - own_z) * other_half

    def slot_late(t):
        across = 2 * (1 - high)
        return (across + 1 - high, across + high, twin, z)[t - quads]

    def slot(t):
        return slot_of(t) if t < quads else slot_late(t)

    def width_of(t):
        return (wide, rest, block)[t // quads]

    def strip(to, px, py):
        r = (to * 4 + py * 2 + px) % half
        own = 1 - (to // 2 - c) * (to // 2 - c)
        return r + (1 - own) * (wrapped // block), r + (1 - own) * c

    def lanes(start, count):
        return pl.ds(pl.multiple_of(start * block, block), count)

    def product(left, right, count):
        rows_at, cols_at = lanes(left, block), lanes(right, count)
        lh, ll = hi[:, rows_at], lo[:, rows_at]
        rh, rl = hi[:, cols_at], lo[:, cols_at]
        return gram(lh, rh) + (gram(lh, rl) + gram(ll, rh))

    def compute(t, side, dst, send=False):
        def body(j, carry):
            b = (1 - second) + j * (2 * second - 1)
            px, py = side * (1 - c) + b * c, b * (1 - c) + side * c
            if t == extra:
                r = py * 2 + px
                late[quads, 0 if send else 1, j, :, :block] = product(r, r + half // 2, block)
            else:
                to = slot_of(t)
                value = product(*strip(to, px, py), wide + rest)
                dst[t, j] = value[:, :wide]
                late[to, 0 if send else 1, j] = value[:, wide:]
            if send:
                stage1(t, j).start()
            return carry

        lax.fori_loop(0, 2, body, 0)

    def remote(src, dst, send, recv, scen, fac):
        return pltpu.make_async_remote_copy(
            src_ref=src, dst_ref=dst, send_sem=send, recv_sem=recv,
            device_id=(scen, fac), device_id_type=MESH,
        )

    def sent(t, j):
        if t < quads:
            return send1.at[t, j]
        return late.at[quads if t == extra else slot_late(t), 0, j, :, :width_of(t)]

    def kept(t, j):
        if t < quads:
            return keep1[t, j]
        return late[quads if t == extra else slot_late(t), 1, j, :, :width_of(t)]

    def stage1(t, j):
        return remote(
            sent(t, j), recv1.at[t, j, :, :width_of(t)], s1_s.at[t // quads // 2], s1_r.at[t, j], peer1, c
        )

    def stage2(t):
        w = width_of(t)
        return remote(send2.at[t, :, :w], recv2.at[t, :, :w], s2_s.at[t // quads // 2], s2_r.at[t], peer2, c)

    def crosses(t):
        if t >= quads:
            return (1, 1, 0)[t - quads], t - quads
        return (1 - own_z, 1, own_z)[t], t - own_z

    def stage3(t):
        w = width_of(t)
        cross, order = crosses(t)
        last = cross * inner
        place = last + cross * (1 - inner) * (2 + order)
        if t < quads:
            src, dst = zpair.at[t], zland.at[place]
        else:
            src, dst = zsend.at[t, :, :w], zrecv.at[place]
        return remote(
            src, dst, z_s.at[t // quads], z_r.at[t // quads, place],
            (last * slot(t) + (1 - last) * twin) * 4 + y * 2 + x, c,
        )

    def from_z(t, place):
        p = t // quads
        to = zrecv.at[place] if p else zland.at[place]
        remote(to, to, z_s.at[p], z_r.at[p, place], s, 1 - c).wait_recv()
        return to[...]

    def relay3(t):
        cross, order = crosses(t)

        @pl.when(cross * inner == 1)
        def _():
            if t < quads:
                zpair[t] = zpair[t] + from_z(t, 2 + order)
            else:
                zsend[t, :, :rest] = zsend[t, :, :rest] + from_z(t, 2 + order)
            stage3(t).start()

    def stage3_extra(e):
        to = 2 * c + e
        place = (z - to + quads - 1) % quads
        return remote(
            zsend.at[extra, :, :block], xrecv.at[place], x_s.at[e], x_r.at[place],
            to * 4 + y * 2 + x, c,
        )

    def with_stage3(t, act, every=False):
        if t == extra:
            for e in range(2):
                pl.when(2 * c + e != z)(act(stage3_extra(e)))
        elif t % quads < quads - 1:
            pl.when((crosses(t)[0] * inner == 0) | every)(act(stage3(t)))

    def relay1(t):
        w = width_of(t)
        if t < quads:
            for j in range(2):
                stage1(t, j).wait_recv()
                zpair[t, j] = keep1[t, j] + recv1[t, j, :, :w]
            if t:
                with_stage3(t, lambda copy: copy.start)
            else:
                pl.when((own_z == 0) & (inner == 0))(stage3(0).start)
            if t == 2:
                pl.when(own_z == 1)(stage3(0).start)
            return
        stage1(t, 0).wait_recv()
        send2[t, :, :w] = kept(t, 0) + recv1[t, 0, :, :w]
        stage2(t).start()

    def join1():
        t = quads - 1
        a, b = from_z(t, 0), from_z(t, 1)
        send2[t, :, :wide] = zpair[t, 0] + a[0] + b[0]
        stage2(t).start()
        zsend[t, :, :wide] = zpair[t, 1] + a[1] + b[1]

    def relay2(t):
        w = width_of(t)
        stage1(t, 1).wait_recv()
        stage2(t).wait_recv()
        zsend[t, :, :w] = kept(t, 1) + recv1[t, 1, :, :w] + recv2[t, :, :w]
        with_stage3(t, lambda copy: copy.start)

    def send_stage(t):
        for j in range(2):
            stage1(t, j).start()

    def pair_copy(i, mine):
        h = own_z * (1 - odd) + (1 - own_z) * c if mine else own_z * (1 - c) + (1 - own_z) * (1 - odd)
        h = h if i < 2 else 1 - h
        at = pl.ds(i % 2 * (rows // 2), rows // 2), pl.ds(pl.multiple_of(h * mid, block), mid)
        return h, remote(x_vm.at[at], other.at[at], pair_s, pair_r.at[i // 2], s, 1 - c)

    def pair_part(half_at):
        h, _ = pair_copy(2 * half_at, False)
        cols = pl.ds(pl.multiple_of(h * mid, block), mid)
        to = other.at[:, cols]
        remote(to, to, pair_s, pair_r.at[half_at], s, 1 - c).wait_recv()
        split(other, pair_sum[:, cols] / rows, cols, wrapped + h * mid, 0, rows, False)

    def mean_copy(d):
        p = (s + d) % n
        return remote(sums_own.at[s], sums_own.at[s], m_s, m_r, p, c)

    pl.semaphore_wait(barrier, 2 * n - 1)
    pair_mean = remote(sums_own.at[s], pair_sum, ps_s, ps_r, s, 1 - c)
    pair_mean.start()
    for i in range(4):
        pair_copy(i, True)[1].start()
    compute(extra, 1 - first, send1, True)
    for d in range(1, n):
        mean_copy(d).start()
    compute(0, 1 - first, send1, True)
    compute(0, first, keep1)
    compute(extra, first, keep1)
    relay1(extra)
    pair_mean.wait_recv()
    pair_part(0)
    compute(1, 1 - first, send1, True)
    compute(1, first, keep1)
    relay1(0)
    relay2(extra)
    pair_part(1)
    compute(2, 1 - first, send1, True)
    compute(2, first, keep1)
    compute(3, 1 - first, send1, True)
    for t in range(quads, 2 * quads):
        send_stage(t)
    relay1(1)
    compute(3, first, keep1)
    relay1(2)
    relay1(3)
    most_sums = sums_own.at[pl.ds(0, n - 1)]
    all_means = remote(most_sums, most_sums, m_s, m_r, s, 1 - c)
    all_means.wait_recv()
    swap = remote(sums_own, sums_oth, mo_s, mo_r, s, 1 - c)
    swap.start()
    relay1(quads + 0)
    relay3(0)
    relay3(1)

    def deviations(ref):
        sums = ref[...].reshape(n, width)
        total = jnp.sum(sums, axis=0, keepdims=True)
        return sums / rows - total / total_rows, total / total_rows

    dev, means = deviations(sums_own)
    mean_ref[...] = means
    dev_a[:, :width] = dev
    dev_a[:, width:wrapped] = dev[:, :mid]
    swap.wait_recv()
    dev_a[:, wrapped:] = deviations(sums_oth)[0]

    r = s % half
    start = r + (1 - own_z) * c

    def put(q, value):
        cov_ref[:, lanes(q % half, block)] = value

    def turn_copy(d):
        return remote(
            turned.at[d], landed.at[d], t_s.at[(d + strip_blocks - 1) // strip_blocks], t_r.at[d],
            c * half + (start + d) % half, own_z * c + (1 - own_z) * (1 - c),
        )

    def mirrored(d, act):
        if d:
            act()
        else:
            pl.when(own_z == 0)(act)

    def finish(p):
        t = p * quads + quads - 1
        w = width_of(t)
        if p:
            arrived = [from_z(t, place) for place in range(2)]
        else:
            stage2(t).wait_recv()
            arrived = [recv2[t, :, :w]]
        left, right = strip(z, x, y)
        right = right + p * AHEAD
        shift = block_gram(dev_a[:, lanes(left, block)], dev_a[:, lanes(right, w)])
        value = zsend[t, :, :w]
        for other_z in arrived:
            value = value + other_z
        value = (value + rows * shift) / (total_rows - 1)
        pieces = piece(p)
        for i, d in enumerate(pieces):
            turned[d] = value[:, i * block:(i + 1) * block].T
            mirrored(d, turn_copy(d).start)
        for i, d in enumerate(pieces):
            put(start + d, value[:, i * block:(i + 1) * block])

    def piece(p):
        return range(AHEAD, strip_blocks) if p else range(AHEAD)

    def land(p):
        for d in piece(p):
            def arrive():
                turn_copy(d).wait_recv()
                put(r - (1 - own_z) * (1 - c) - d + 2 * half, landed[d])

            mirrored(d, arrive)

    def finish_extra():
        @pl.when(own_z == 1)
        def _():
            for place in range(quads - 1):
                remote(
                    zsend.at[extra, :, :block], xrecv.at[place], x_s.at[0], x_r.at[place], s, 1 - c
                ).wait_recv()
            left = y * 2 + x
            shift = block_gram(
                dev_a[:, lanes(left, block)], dev_a[:, lanes(left + half // 2, block)]
            )
            value = zsend[extra, :, :block]
            for place in range(quads - 1):
                value = value + xrecv[place]
            value = (value + rows * shift) / (total_rows - 1)

            @pl.when(odd == 0)
            def _():
                put(r + half // 2, value)

            @pl.when(odd == 1)
            def _():
                put(r + half // 2, value.T)

    relay1(quads + 1)
    relay2(quads + 0)
    relay3(2)
    relay1(quads + 2)
    relay2(quads + 1)
    relay3(quads + 0)
    join1()
    relay1(quads + 3)
    relay2(quads + 2)
    relay3(quads + 1)
    finish(0)
    finish_extra()
    relay2(quads + 3)
    finish(1)
    land(0)
    land(1)

    def sent_bytes(ref, sem):
        remote(ref, ref, sem, ps_r, s, 1 - c).wait_send()

    pair_mean.wait_send()
    swap.wait_send()
    sent_bytes(other, pair_s)
    all_means.wait_send()
    for d in range(min(2, strip_blocks)):
        pl.when((d == 1) | (own_z == 0))(
            functools.partial(
                sent_bytes, landed.at[pl.ds(d, (1, strip_blocks - 1)[d])], t_s.at[d]
            )
        )
    sent_bytes(send1, s1_s.at[0])
    sent_bytes(late.at[pl.ds(0, quads), 1], s1_s.at[0])
    sent_bytes(late.at[quads, 1, :, :, :block], s1_s.at[1])
    sent_bytes(recv2.at[quads - 1, :, :wide], s2_s.at[0])
    sent_bytes(recv2.at[pl.ds(quads, quads), :, :rest], s2_s.at[0])
    sent_bytes(recv2.at[extra, :, :block], s2_s.at[1])
    sent_bytes(zpair.at[pl.ds(0, quads - 1)], z_s.at[0])
    sent_bytes(zsend.at[pl.ds(quads, quads - 1), :, :rest], z_s.at[1])
    with_stage3(extra, lambda copy: copy.wait_send)


def by_kernel(n, scenario_pnl):
    rows, width = scenario_pnl.shape
    half = n // 2
    block = width // half
    wide, rest = AHEAD * block, (half // 2 - AHEAD) * block
    most = max(wide, rest)
    tasks = 2 * (n // 4) + 1
    f32, bf16 = jnp.float32, jnp.bfloat16
    dma = pltpu.SemaphoreType.DMA
    covariance, factor_means = pl.pallas_call(
        functools.partial(kernel, n),
        out_shape=(pltpu.VMEM((block, width), f32), pltpu.VMEM((1, width), f32)),
        in_specs=[pl.BlockSpec(memory_space=pl.ANY)],
        out_specs=[pl.BlockSpec(memory_space=pltpu.VMEM)] * 2,
        scratch_shapes=[
            pltpu.VMEM((rows, width), f32),
            pltpu.VMEM((rows, width), f32),
            pltpu.VMEM((rows, 2 * width + width // 2), bf16),
            pltpu.VMEM((rows, 2 * width + width // 2), bf16),
            pltpu.VMEM((n // 4, 2, block, wide), f32),
            pltpu.VMEM((n // 4, 2, block, wide), f32),
            pltpu.VMEM((tasks, 2, block, most), f32),
            pltpu.VMEM((tasks, block, most), f32),
            pltpu.VMEM((tasks, block, most), f32),
            pltpu.VMEM((n // 4, 2, block, wide), f32),
            pltpu.VMEM((4, 2, block, wide), f32),
            pltpu.VMEM((tasks, block, most), f32),
            pltpu.VMEM((4, block, rest), f32),
            pltpu.VMEM((3, block, block), f32),
            pltpu.VMEM((n // 4 + 1, 2, 2, block, rest), f32),
            pltpu.VMEM((half // 2, block, block), f32),
            pltpu.VMEM((half // 2, block, block), f32),
            pltpu.VMEM((n, 1, width), f32),
            pltpu.VMEM((n, 1, width), f32),
            pltpu.VMEM((1, width), f32),
            pltpu.VMEM((n, 2 * width + width // 2), f32),
            dma((LOADS,)),
            dma, dma((2,)),
            dma, dma,
            dma((2,)), dma((tasks, 2)),
            dma((2,)), dma((tasks,)),
            dma((2,)), dma((2, 4)),
            dma((2,)), dma((3,)),
            dma((2,)), dma((half // 2,)),
            dma, dma,
            dma, dma,
        ],
        compiler_params=pltpu.CompilerParams(
            collective_id=0, has_side_effects=True, vmem_limit_bytes=60 * 1024 * 1024
        ),
    )(scenario_pnl)
    return covariance, factor_means.reshape(width)


def solution(mesh):
    n, cores = mesh.shape["scen"], mesh.shape["fac"]

    def body(scenario_pnl):
        rows, width = scenario_pnl.shape
        fits = cores == 2 and n % 16 == 0 and n // 4 == 4 and width % (n * 64) == 0
        if fits and rows % (LOADS * TILE) == 0:
            return by_kernel(n, scenario_pnl)
        return on_device(scenario_pnl)

    return jax.shard_map(
        body,
        mesh=mesh,
        in_specs=(P("scen", "fac"),),
        out_specs=(P("scen", "fac"), P("fac")),
        check_vma=False,
    )
```
